32 devices in a mesh: section: 4 (over z), fsdp: 4 (over y, core), tp: 2 (over x).
Axes of the slice: x: 2, y: 2, z: 4, core: 2. Of those that a mesh axis runs over, the one named last changes fastest.
Arguments:
- stash: bfloat16 [4, 4, 512, 2304], P('section', None, 'fsdp'), may hold values from -6 to 6
- grad_now: bfloat16 [4, 512, 2304], P('section', 'fsdp'), may hold values from -6 to 6
- grad_top: bfloat16 [2, 512, 2304], P(None, 'fsdp'), may hold values from -6 to 6
- order: int32 [4, 4], P('section'), may hold values from 0 to 3, each once within a row
- gain: float32 [4, 2304], P('section'), may hold values from 0.5 to 1.5
- weight: bfloat16 [4, 2304, 2048], P('section', 'fsdp', 'tp'), may hold values from -0.125 to 0.125
Outputs:
- grad_held: bfloat16 [4, 512, 2304], P('section', 'fsdp')
- weight_grad: float32 [4, 2304, 2048], P('section', 'fsdp', 'tp')
The draws below stay inside these ranges and needn't reach their ends.
Inputs may be any that keep to these rules, and one draw needn't show every extreme that they name: Each row of order names every kept micro-batch once.
All inputs are finite; a program needn't handle non-finite values.
Results may differ from the reference program's by a relative error of at most 0.013.
Values may be sent and summed in bfloat16 or wider, within the bound.
A program may use at most 64 MiB of HBM per device.

```python
import jax
import jax.numpy as jnp
from jax import lax

D = 2304
INNER = 2048
MB = 4
TICKS = 2
SECTIONS = 4
TOKENS = 512
N_TP = 2


def level_of(key, extent, pieces, least, largest):
    def one(axis_at, blocks):
        heights = jax.random.uniform(jax.random.fold_in(jax.random.fold_in(key, 6), axis_at), (blocks,), jnp.float32, least / len(pieces), largest / len(pieces))
        return jnp.repeat(jnp.exp(heights), extent[axis_at] // blocks).reshape((-1,) + (1,) * (len(extent) - axis_at - 1))

    level = one(*pieces[0])
    for cut in pieces[1:]:
        level = level * one(*cut)
    return level


def scatter_about(key, extent, spread, limit, cuts=(), kind=jnp.bfloat16):
    loudness = level_of(key, extent, cuts, -0.22, 0.18) if cuts else 1.0
    drawn = jax.random.normal(key, extent, jnp.float32) * spread * loudness
    return jnp.minimum(jnp.maximum(drawn, -limit), limit).astype(kind)


def setup_inputs(seed: int = 0) -> dict:
    seeds = jax.random.split(jax.random.key(seed), 7)
    stash = scatter_about(seeds[0], (SECTIONS, MB, TOKENS, D), 1.0, 6.0, ((0, 4), (2, 4)))
    grad_now = scatter_about(seeds[1], (SECTIONS, TOKENS, D), 1.0, 6.0, ((0, 4), (1, 4)))
    grad_top = scatter_about(seeds[2], (TICKS, TOKENS, D), 1.0, 6.0, ((1, 4),))
    order = jax.vmap(lambda own: jax.random.permutation(own, MB))(jax.random.split(seeds[3], SECTIONS)).reshape((SECTIONS, MB)).astype(jnp.int32)
    gain = jnp.clip(1.0 + 0.1 * jax.random.normal(seeds[4], (SECTIONS, D), jnp.float32), 0.5, 1.5)
    weight = scatter_about(seeds[5], (SECTIONS, D, INNER), D ** -0.5, 0.125, ((0, 4), (1, 4), (2, 2)))
    return dict(stash=stash, grad_now=grad_now, grad_top=grad_top, order=order, gain=gain, weight=weight)


norm_eps = 1e-06

def gelu_tanh(values):
    return jax.nn.gelu(values, approximate=True)

def section_tick(section_in, grad_in, section_gain, section_weight):
    values = section_in.astype(jnp.float32)
    inv_rms = lax.rsqrt(lax.optimization_barrier(jnp.mean(values * values, axis=-1, keepdims=True)) + norm_eps)
    scaled = values * inv_rms
    normed = (scaled * section_gain).astype(jnp.bfloat16)
    hidden = jnp.dot(normed, section_weight, preferred_element_type=jnp.float32)
    backed = jnp.dot(grad_in, section_weight, preferred_element_type=jnp.float32)
    activated, pullback = jax.vjp(gelu_tanh, hidden)
    grad_pre = pullback(backed)[0].astype(jnp.bfloat16)
    activated = activated.astype(jnp.bfloat16)
    group = section_weight.shape[1] // N_TP
    total = jnp.zeros(values.shape, jnp.float32)
    for member in range(N_TP):
        left = grad_pre[:, member * group:(member + 1) * group]
        right = section_weight[:, member * group:(member + 1) * group]
        partial_dh = lax.dot_general(left, right, (((1,), (1,)), ((), ())), preferred_element_type=jnp.float32)
        rounded = lax.optimization_barrier(partial_dh.astype(jnp.bfloat16))
        total = total + rounded.astype(jnp.float32)
    gained = section_gain * total
    inner_mean = lax.optimization_barrier(jnp.mean(gained * scaled, axis=-1, keepdims=True))
    grad_out = (grad_in.astype(jnp.float32) + inv_rms * (gained - scaled * inner_mean)).astype(jnp.bfloat16)
    return (grad_out, normed, grad_pre, activated)

def reference(stash, grad_now, grad_top, order, gain, weight):
    held = grad_now
    lhs_parts = []
    rhs_parts = []
    for tick_id in range(TICKS):

        def per_section(items):
            section_stash, section_order, grad_in, section_gain, section_weight = items
            slot_id = section_order[tick_id].astype(jnp.int32)
            section_in = lax.dynamic_index_in_dim(section_stash, slot_id, 0, keepdims=False)
            return section_tick(section_in, grad_in, section_gain, section_weight)
        grad_out, normed, grad_pre, activated = lax.map(per_section, (stash, order, held, gain, weight))
        lhs_parts.append(normed)
        lhs_parts.append(held)
        rhs_parts.append(grad_pre)
        rhs_parts.append(activated)
        held = jnp.concatenate([grad_out[1:], grad_top[tick_id][None]], axis=0)
    lhs_all = jnp.concatenate(lhs_parts, axis=1)
    rhs_all = jnp.concatenate(rhs_parts, axis=1)

    def section_grad(items):
        left, right = items
        return lax.dot_general(left, right, (((0,), (0,)), ((), ())), preferred_element_type=jnp.float32)
    weight_grad = lax.map(section_grad, (lhs_all, rhs_all))
    return (held, weight_grad)
```

```python
import functools

import jax
import jax.numpy as jnp
from jax import lax
from jax.experimental import pallas as pl
from jax.experimental.pallas import tpu as pltpu
from jax.sharding import PartitionSpec as P

norm_eps = 1e-06
MESH = pl.DeviceIdType.MESH
f32 = jnp.float32
bf16 = jnp.bfloat16
LAG = 2


def gelu_parts(u):
    k = 0.7978845608028654
    c = 0.044715
    u2 = u * u
    t = jnp.tanh(k * u * (1.0 + c * u2))
    half = 0.5 * (1.0 + t)
    act = u * half
    slope = half + 0.5 * u * (1.0 - t * t) * (k * (1.0 + 3.0 * c * u2))
    return act, slope


def pick(extent, options):
    for o in options:
        if extent % o == 0:
            return o
    return extent


def kernel(
    S, FS, TP, T, order_ref, gain_ref, stash_ref, gnow_ref, gtop_ref, w_ref,
    held_ref, wg_ref,
    wfull, stash, act, xt, inv, dyn, lt, lta, rhs, prod, slope, own_e, peer_e, dxs, acc,
    lsem, topsem, ownsem, heldsem, w_s, w_r, l_s, l_r, r_s, r_r, e_s, e_r, z_s, z_r,
):
    s = lax.axis_index("section")
    f = lax.axis_index("fsdp")
    p = lax.axis_index("tp")
    NC = FS // 2
    yc = f // 2
    core = f % 2
    sib = 2 * yc + (1 - core)
    n, D = act.shape[0] // (T + 1), act.shape[1]
    wl, N = w_ref.shape[1], w_ref.shape[2]
    WCH = w_s.shape[1]
    wc = wl // WCH
    CW = D // e_s.shape[-1]
    CH = D // CW
    nw = pick(N, (256, 128))

    loads = [
        pltpu.make_async_copy(w_ref.at[0], wfull.at[pl.ds(f * wl, wl), :], lsem.at[0]),
        pltpu.make_async_copy(stash_ref.at[0], stash, lsem.at[1]),
        pltpu.make_async_copy(gnow_ref.at[0], act.at[pl.ds(T * n, n), :], lsem.at[2]),
    ]
    for c in loads:
        c.start()

    bar = pltpu.get_barrier_semaphore()
    for r in range(1, FS):
        pl.semaphore_signal(bar, inc=1, device_id={"fsdp": (f + r) % FS}, device_id_type=MESH)
    for r in range(1, TP):
        pl.semaphore_signal(bar, inc=1, device_id={"tp": (p + r) % TP}, device_id_type=MESH)

    @pl.when(s > 0)
    def _():
        pl.semaphore_signal(bar, inc=1, device_id={"section": s - 1}, device_id_type=MESH)

    @pl.when(s < S - 1)
    def _():
        pl.semaphore_signal(bar, inc=1, device_id={"section": s + 1}, device_id_type=MESH)

    pl.semaphore_wait(bar, FS - 1 + TP - 1 + jnp.minimum(s, 1) + jnp.minimum(S - 1 - s, 1))

    def rcopy(src, dst, ss, rs, dev):
        return pltpu.make_async_remote_copy(
            src_ref=src, dst_ref=dst, send_sem=ss, recv_sem=rs, device_id=dev, device_id_type=MESH
        )

    def w_copy(k, j):
        if k < NC:
            rows = pl.ds(f * wl + j * wc, wc)
            src = w_ref.at[0, pl.ds(j * wc, wc), :]
            to = sib if k == 0 else 2 * ((yc + k) % NC) + core
        else:
            o = k - NC + 1
            rows = pl.ds((2 * ((yc - o + NC) % NC) + core) * wl + j * wc, wc)
            src = wfull.at[rows, :]
            to = sib
        return rcopy(src, wfull.at[rows, :], w_s.at[k, j], w_r.at[k, j], {"fsdp": to})

    for k in list(range(1, NC)) + [0]:
        for j in range(WCH):
            w_copy(k, j).start()

    def l_copy(part, r):
        to = (f + r) % FS
        return rcopy(
            lt.at[part, pl.ds(to * wl, wl), :], lta.at[part, :, pl.ds(pl.multiple_of(f * n, n), n)],
            l_s.at[part, r - 1], l_r.at[part, r - 1], {"fsdp": to},
        )

    def l_own(part):
        return pltpu.make_async_copy(
            lt.at[part, pl.ds(f * wl, wl), :], lta.at[part, :, pl.ds(pl.multiple_of(f * n, n), n)],
            ownsem.at[part],
        )

    def l_send(part):
        for r in range(1, FS):
            l_copy(part, r).start()
        l_own(part).start()

    def r_copy(part, k):
        if k < NC:
            at = f
            to = sib if k == 0 else 2 * ((yc + k) % NC) + core
        else:
            o = k - NC + 1
            at = 2 * ((yc - o + NC) % NC) + core
            to = sib
        blk = rhs.at[part, pl.ds(pl.multiple_of(at * n, n), n), :]
        return rcopy(blk, blk, r_s.at[part, k], r_r.at[part, k], {"fsdp": to})

    def r_send(part):
        for k in list(range(1, NC)) + [0]:
            r_copy(part, k).start()

    tw = pick(D, (256, 128))

    def transpose_rows(part, ref, first):
        @pl.loop(0, D // tw)
        def _(i):
            cols = pl.ds(pl.multiple_of(i * tw, tw), tw)
            lt[part, cols, :] = ref[pl.ds(first, n), cols].astype(f32).T.astype(bf16)

    loads[1].wait()
    rb = pick(n, (32, 16))
    for t in range(T):
        slot = order_ref[0, t]

        @pl.loop(0, n // rb)
        def _(i):
            rows = pl.ds(pl.multiple_of(i * rb, rb), rb)
            raw = stash[slot, rows, :]
            v = raw.astype(f32)
            iv = lax.rsqrt(jnp.mean(v * v, axis=-1, keepdims=True) + norm_eps)
            xt[t, rows, :] = raw
            inv[t, rows, :] = jnp.broadcast_to(iv, (rb, 128))
            act[pl.ds(pl.multiple_of(t * n + i * rb, rb), rb), :] = ((v * iv) * gain_ref[0:1, :]).astype(bf16)

        transpose_rows(2 * t, act, t * n)
        if t == 0:
            l_send(0)
            loads[2].wait()
            transpose_rows(1, act, T * n)
            l_send(1)
        else:
            l_send(2 * t)

    @pl.when(s == S - 1)
    def _():
        for t in range(T):
            pltpu.make_async_copy(gtop_ref.at[t], dyn.at[t], topsem.at[t]).start()

    half = 2 * wl

    def part_product(chip, first):
        ks = pl.ds(pl.multiple_of(chip * half, half), half)

        @pl.loop(0, N // nw)
        def _(i):
            cols = pl.ds(pl.multiple_of(i * nw, nw), nw)
            d = jnp.dot(act[:, ks], wfull[ks, cols], preferred_element_type=f32)
            if first:
                prod[:, cols] = d
            else:
                prod[:, cols] += d

    loads[0].wait()
    for j in range(WCH):
        w_copy(0, j).wait_recv()
    part_product(yc, True)
    for o in range(1, NC):
        for j in range(WCH):
            w_copy(o, j).wait_recv()
            w_copy(NC - 1 + o, j).start()
        for j in range(WCH):
            w_copy(NC - 1 + o, j).wait_recv()
        part_product((yc - o + NC) % NC, False)

    mine = pl.multiple_of(f * n, n)

    def gelu_rows(t, with_grad):
        @pl.loop(0, n // rb)
        def _(i):
            rows = pl.ds(pl.multiple_of(t * n + i * rb, rb), rb)
            here = pl.ds(pl.multiple_of(mine + i * rb, rb), rb)
            a, sl = gelu_parts(prod[rows, :])
            rhs[2 * t + 1, here, :] = a.astype(bf16)
            if with_grad:
                g = prod[pl.ds(pl.multiple_of(T * n + i * rb, rb), rb), :]
                rhs[2 * t, here, :] = (sl * g).astype(bf16)
            else:
                slope[t, pl.ds(pl.multiple_of(i * rb, rb), rb), :] = sl

    def e_copy(t, r, c):
        cols = pl.ds(pl.multiple_of(c * CW, CW), CW)
        return rcopy(
            own_e.at[t, :, cols], peer_e.at[t, r - 1, :, cols],
            e_s.at[t, r - 1, c], e_r.at[t, r - 1, c], {"tp": (p + r) % TP},
        )

    def z_copy(t, c):
        cols = pl.ds(pl.multiple_of(c * CW, CW), CW)
        to = jnp.maximum(s - 1, 0)
        return rcopy(
            dxs.at[t, :, cols], dyn.at[t, :, cols], z_s.at[t, c], z_r.at[t, c], {"section": to}
        )

    def spread(t):
        du = rhs[2 * t, pl.ds(mine, n), :]
        u = prod[pl.ds(t * n, n), :]
        m = jnp.sum(du.astype(f32) * u, axis=-1, keepdims=True) / D
        iv = inv[t, :, 0:1]
        q_scale = iv * iv * m

        @pl.loop(0, CH)
        def _(c):
            cols = pl.ds(pl.multiple_of(c * CW, CW), CW)
            dh = lax.dot_general(
                rhs[2 * t, pl.ds(mine, n), :], wfull[cols, :], (((1,), (1,)), ((), ())),
                preferred_element_type=f32,
            )
            e = iv * (gain_ref[0:1, cols] * dh) - xt[t, :, cols].astype(f32) * q_scale
            own_e[t, :, cols] = e.astype(bf16)
            for r in range(1, TP):
                e_copy(t, r, c).start()

    def combine(t, c):
        cols = pl.ds(pl.multiple_of(c * CW, CW), CW)
        for r in range(1, TP):
            e_copy(t, r, c).wait_recv()
        total = own_e[t, :, cols].astype(f32)
        for r in range(1, TP):
            total = total + peer_e[t, r - 1, :, cols].astype(f32)
        dy = act[pl.ds(T * n, n), cols] if t == 0 else dyn[t - 1, :, cols]
        dxs[t, :, cols] = (dy.astype(f32) + total).astype(bf16)
        z_copy(t, c).start()

    for t in range(T):
        if t == 0:
            gelu_rows(0, True)
        r_ids = [0, 1] if t == 0 else [2 * t]

        @pl.when(s > 0)
        def _():
            spread(t)

        for part in r_ids:
            r_send(part)
        if t == 0:
            for later in range(1, T):
                gelu_rows(later, False)
                r_send(2 * later + 1)

        if t < T - 1:
            @pl.when(s == S - 1)
            def _():
                pltpu.make_async_copy(gtop_ref.at[t], dyn.at[t], topsem.at[t]).wait()

            gr = pl.ds(T * n, n)

            @pl.loop(0, CH + LAG)
            def _(i):
                @pl.when((i < CH) & (s > 0))
                def _():
                    combine(t, i)

                @pl.when(i >= LAG)
                def _():
                    c = i - LAG

                    @pl.when(s < S - 1)
                    def _():
                        z_copy(t, c).wait_recv()

                    cols = pl.ds(pl.multiple_of(c * CW, CW), CW)
                    d = dyn[t, :, cols]
                    lt[2 * t + 3, cols, :] = d.astype(f32).T.astype(bf16)
                    g = jnp.dot(d, wfull[cols, :], preferred_element_type=f32)

                    @pl.when(c == 0)
                    def _():
                        prod[gr, :] = g

                    @pl.when(c > 0)
                    def _():
                        prod[gr, :] += g

            l_send(2 * t + 3)

            @pl.loop(0, n // rb)
            def _(i):
                rows = pl.ds(pl.multiple_of(i * rb, rb), rb)
                g = prod[pl.ds(pl.multiple_of(T * n + i * rb, rb), rb), :]
                here = pl.ds(pl.multiple_of(mine + i * rb, rb), rb)
                rhs[2 * t + 2, here, :] = (slope[t + 1, rows, :] * g).astype(bf16)
        else:
            @pl.when(s > 0)
            def _():
                @pl.loop(0, CH)
                def _(c):
                    combine(t, c)

    parts = []
    for t in range(T):
        parts += [2 * t, 2 * t + 1] if t == 0 else [2 * t + 1, 2 * t]
    for at, part in enumerate(parts):
        l_own(part).wait()
        for r in range(1, FS):
            l_copy(part, r).wait_recv()
        for o in range(1, NC):
            r_copy(part, o).wait_recv()
            r_copy(part, NC - 1 + o).start()
        r_copy(part, 0).wait_recv()
        for o in range(1, NC):
            r_copy(part, NC - 1 + o).wait_recv()
        final = at == len(parts) - 1

        @pl.loop(0, N // nw)
        def _(i):
            cols = pl.ds(pl.multiple_of(i * nw, nw), nw)
            d = jnp.dot(lta[part], rhs[part, :, cols], preferred_element_type=f32)
            if at > 0:
                d = acc[:, cols] + d
            if final:
                wg_ref[0, :, cols] = d.astype(bf16)
            else:
                acc[:, cols] = d

    t = T - 1

    @pl.when(s == S - 1)
    def _():
        pltpu.make_async_copy(gtop_ref.at[t], dyn.at[t], topsem.at[t]).wait()

    @pl.when(s < S - 1)
    def _():
        @pl.loop(0, CH)
        def _(c):
            z_copy(t, c).wait_recv()

    out = pltpu.make_async_copy(dyn.at[t], held_ref.at[0], heldsem.at[0])
    out.start()

    for j in range(WCH):
        for k in range(2 * NC - 1):
            w_copy(k, j).wait_send()
    for part in range(2 * T):
        for r in range(1, FS):
            l_copy(part, r).wait_send()
        for k in range(2 * NC - 1):
            r_copy(part, k).wait_send()

    @pl.when(s > 0)
    def _():
        for t in range(T):
            @pl.loop(0, CH)
            def _(c):
                for r in range(1, TP):
                    e_copy(t, r, c).wait_send()
                z_copy(t, c).wait_send()

    out.wait()


def solution(mesh):
    S, FS, TP = mesh.shape["section"], mesh.shape["fsdp"], mesh.shape["tp"]

    def per_device(stash, grad_now, grad_top, order, gain, weight):
        MB, n, D = stash.shape[1:]
        T = grad_top.shape[0]
        wl, N = weight.shape[1:]
        NC = FS // 2
        CH = D // pick(D, (384, 256, 128))
        WCH = 4 if wl % 64 == 0 else 1
        K = 2 * NC - 1
        DMA = pltpu.SemaphoreType.DMA
        V = pltpu.VMEM
        any_ = pl.BlockSpec(memory_space=pl.ANY)
        peers = max(TP - 1, 1)
        held, wg = pl.pallas_call(
            functools.partial(kernel, S, FS, TP, T),
            out_shape=(
                jax.ShapeDtypeStruct((1, n, D), bf16),
                jax.ShapeDtypeStruct((1, wl, N), bf16),
            ),
            in_specs=[
                pl.BlockSpec(memory_space=pltpu.SMEM),
                pl.BlockSpec(memory_space=pltpu.VMEM),
                any_, any_, any_, any_,
            ],
            out_specs=(any_, pl.BlockSpec(memory_space=pltpu.VMEM)),
            scratch_shapes=[
                V((FS * wl, N), bf16),
                V((MB, n, D), bf16),
                V(((T + 1) * n, D), bf16),
                V((T, n, D), bf16),
                V((T, n, 128), f32),
                V((T, n, D), bf16),
                V((2 * T, D, n), bf16),
                V((2 * T, wl, FS * n), bf16),
                V((2 * T, FS * n, N), bf16),
                V(((T + 1) * n, N), f32),
                V((T, n, N), f32),
                V((T, n, D), bf16),
                V((T, peers, n, D), bf16),
                V((T, n, D), bf16),
                V((wl, N), f32),
                DMA((3,)), DMA((T,)), DMA((2 * T,)), DMA((1,)),
                DMA((K, WCH)), DMA((K, WCH)),
                DMA((2 * T, FS - 1)), DMA((2 * T, FS - 1)),
                DMA((2 * T, K)), DMA((2 * T, K)),
                DMA((T, peers, CH)), DMA((T, peers, CH)),
                DMA((T, CH)), DMA((T, CH)),
            ],
            compiler_params=pltpu.CompilerParams(
                collective_id=0, has_side_effects=True, vmem_limit_bytes=60 * 1024 * 1024
            ),
        )(order, gain, stash, grad_now, grad_top, weight)
        return held, wg.astype(f32)

    return jax.shard_map(
        per_device,
        mesh=mesh,
        in_specs=(
            P("section", None, "fsdp", None),
            P("section", "fsdp", None),
            P(None, "fsdp", None),
            P("section", None),
            P("section", None),
            P("section", "fsdp", "tp"),
        ),
        out_specs=(P("section", "fsdp", None), P("section", "fsdp", "tp")),
        check_vma=False,
    )
```

```python
import functools

import jax
import jax.numpy as jnp
from jax import lax
from jax.experimental import pallas as pl
from jax.experimental.pallas import tpu as pltpu
from jax.sharding import PartitionSpec as P

norm_eps = 1e-06
MESH = pl.DeviceIdType.MESH
f32 = jnp.float32
bf16 = jnp.bfloat16
LAG = 2


def gelu_parts(u):
    k = 0.7978845608028654
    c = 0.044715
    u2 = u * u
    t = jnp.tanh(k * u * (1.0 + c * u2))
    half = 0.5 * (1.0 + t)
    act = u * half
    slope = half + 0.5 * u * (1.0 - t * t) * (k * (1.0 + 3.0 * c * u2))
    return act, slope


def pick(extent, options):
    for o in options:
        if extent % o == 0:
            return o
    return extent


def kernel(
    S, FS, TP, T, order_ref, gain_ref, stash_ref, gnow_ref, gtop_ref, w_ref,
    held_ref, wg_ref,
    wfull, stash, act, xt, inv, dyn, lt, lta, rhs, prod, slope, own_e, peer_e, dxs, acc,
    lsem, topsem, ownsem, heldsem, w_s, w_r, l_s, l_r, r_s, r_r, e_s, e_r, z_s, z_r, x_s, x_r,
):
    s = lax.axis_index("section")
    f = lax.axis_index("fsdp")
    p = lax.axis_index("tp")
    NC = FS // 2
    yc = f // 2
    core = f % 2
    sib = 2 * yc + (1 - core)
    n, D = act.shape[0] // (T + 1), act.shape[1]
    wl, N = w_ref.shape[1], w_ref.shape[2]
    WCH = w_s.shape[1]
    wq = wl // TP
    SPLIT = tuple(2 * t for t in range(T)) + (1,)
    wc = wl // WCH
    CW = D // e_s.shape[-1]
    CH = D // CW
    nw = pick(N, (256, 128))

    loads = [
        pltpu.make_async_copy(w_ref.at[0], wfull.at[pl.ds(f * wl, wl), :], lsem.at[0]),
        pltpu.make_async_copy(stash_ref.at[0], stash, lsem.at[1]),
        pltpu.make_async_copy(gnow_ref.at[0], act.at[pl.ds(T * n, n), :], lsem.at[2]),
    ]
    for c in loads:
        c.start()

    bar = pltpu.get_barrier_semaphore()
    for r in range(1, FS):
        pl.semaphore_signal(bar, inc=1, device_id={"fsdp": (f + r) % FS}, device_id_type=MESH)
    for r in range(1, TP):
        pl.semaphore_signal(bar, inc=1, device_id={"tp": (p + r) % TP}, device_id_type=MESH)

    @pl.when(s > 0)
    def _():
        pl.semaphore_signal(bar, inc=1, device_id={"section": s - 1}, device_id_type=MESH)

    @pl.when(s < S - 1)
    def _():
        pl.semaphore_signal(bar, inc=1, device_id={"section": s + 1}, device_id_type=MESH)

    pl.semaphore_wait(bar, FS - 1 + TP - 1 + jnp.minimum(s, 1) + jnp.minimum(S - 1 - s, 1))

    def rcopy(src, dst, ss, rs, dev):
        return pltpu.make_async_remote_copy(
            src_ref=src, dst_ref=dst, send_sem=ss, recv_sem=rs, device_id=dev, device_id_type=MESH
        )

    def w_copy(k, j):
        if k < NC:
            rows = pl.ds(f * wl + j * wc, wc)
            src = w_ref.at[0, pl.ds(j * wc, wc), :]
            to = sib if k == 0 else 2 * ((yc + k) % NC) + core
        else:
            o = k - NC + 1
            rows = pl.ds((2 * ((yc - o + NC) % NC) + core) * wl + j * wc, wc)
            src = wfull.at[rows, :]
            to = sib
        return rcopy(src, wfull.at[rows, :], w_s.at[k, j], w_r.at[k, j], {"fsdp": to})

    for k in list(range(1, NC)) + [0]:
        for j in range(WCH):
            w_copy(k, j).start()

    def is_split(part):
        return part in SPLIT and TP > 1

    def l_copy(part, k):
        cols = pl.ds(pl.multiple_of(f * n, n), n)
        if k == 0:
            to = sib
        else:
            o, cc = (k + 1) // 2, (k - 1) % 2
            to = 2 * ((yc + o) % NC) + (core + cc) % 2
        if k > 0 and is_split(part):
            src = lt.at[part, pl.ds(to * wl + p * wq, wq), :]
            dst = lta.at[part, pl.ds(p * wq, wq), cols]
        else:
            src = lt.at[part, pl.ds(to * wl, wl), :]
            dst = lta.at[part, :, cols]
        return rcopy(src, dst, l_s.at[part, k], l_r.at[part, k], {"fsdp": to})

    def x_copy(part, k, q):
        o, cc = (k + 1) // 2, (k - 1) % 2
        src_f = 2 * ((yc - o + NC) % NC) + (core + cc) % 2
        blk = lta.at[part, pl.ds(p * wq, wq), pl.ds(pl.multiple_of(src_f * n, n), n)]
        return rcopy(blk, blk, x_s.at[part, k - 1, q - 1], x_r.at[part, k - 1, q - 1], {"tp": (p + q) % TP})

    passed = set()

    def l_pass(part):
        if part in passed or not is_split(part):
            return
        passed.add(part)
        for k in range(1, FS - 1):
            l_copy(part, k).wait_recv()
            for q in range(1, TP):
                x_copy(part, k, q).start()

    def l_own(part):
        return pltpu.make_async_copy(
            lt.at[part, pl.ds(f * wl, wl), :], lta.at[part, :, pl.ds(pl.multiple_of(f * n, n), n)],
            ownsem.at[part],
        )

    def l_send(part):
        for k in list(range(1, FS - 1)) + [0]:
            l_copy(part, k).start()
        l_own(part).start()

    def r_copy(part, k):
        if k < NC:
            at = f
            to = sib if k == 0 else 2 * ((yc + k) % NC) + core
        else:
            o = k - NC + 1
            at = 2 * ((yc - o + NC) % NC) + core
            to = sib
        blk = rhs.at[part, pl.ds(pl.multiple_of(at * n, n), n), :]
        return rcopy(blk, blk, r_s.at[part, k], r_r.at[part, k], {"fsdp": to})

    def r_send(part):
        for k in list(range(1, NC)) + [0]:
            r_copy(part, k).start()

    tw = pick(D, (256, 128))

    def transpose_rows(part, ref, first):
        @pl.loop(0, D // tw)
        def _(i):
            cols = pl.ds(pl.multiple_of(i * tw, tw), tw)
            lt[part, cols, :] = ref[pl.ds(first, n), cols].astype(f32).T.astype(bf16)

    loads[1].wait()
    rb = pick(n, (32, 16))
    for t in range(T):
        slot = order_ref[0, t]

        @pl.loop(0, n // rb)
        def _(i):
            rows = pl.ds(pl.multiple_of(i * rb, rb), rb)
            raw = stash[slot, rows, :]
            v = raw.astype(f32)
            iv = lax.rsqrt(jnp.mean(v * v, axis=-1, keepdims=True) + norm_eps)
            xt[t, rows, :] = raw
            inv[t, rows, :] = jnp.broadcast_to(iv, (rb, 128))
            act[pl.ds(pl.multiple_of(t * n + i * rb, rb), rb), :] = ((v * iv) * gain_ref[0:1, :]).astype(bf16)

        transpose_rows(2 * t, act, t * n)
        if t == 0:
            l_send(0)
            loads[2].wait()
            transpose_rows(1, act, T * n)
            l_send(1)
        else:
            l_send(2 * t)

    @pl.when(s == S - 1)
    def _():
        for t in range(T):
            pltpu.make_async_copy(gtop_ref.at[t], dyn.at[t], topsem.at[t]).start()

    half = 2 * wl

    def part_product(chip, first):
        ks = pl.ds(pl.multiple_of(chip * half, half), half)

        @pl.loop(0, N // nw)
        def _(i):
            cols = pl.ds(pl.multiple_of(i * nw, nw), nw)
            d = jnp.dot(act[:, ks], wfull[ks, cols], preferred_element_type=f32)
            if first:
                prod[:, cols] = d
            else:
                prod[:, cols] += d

    loads[0].wait()
    for j in range(WCH):
        w_copy(0, j).wait_recv()
    part_product(yc, True)
    for o in range(1, NC):
        for j in range(WCH):
            w_copy(o, j).wait_recv()
            w_copy(NC - 1 + o, j).start()
        for j in range(WCH):
            w_copy(NC - 1 + o, j).wait_recv()
        part_product((yc - o + NC) % NC, False)

    mine = pl.multiple_of(f * n, n)

    def gelu_rows(t, with_grad):
        @pl.loop(0, n // rb)
        def _(i):
            rows = pl.ds(pl.multiple_of(t * n + i * rb, rb), rb)
            here = pl.ds(pl.multiple_of(mine + i * rb, rb), rb)
            a, sl = gelu_parts(prod[rows, :])
            rhs[2 * t + 1, here, :] = a.astype(bf16)
            if with_grad:
                g = prod[pl.ds(pl.multiple_of(T * n + i * rb, rb), rb), :]
                rhs[2 * t, here, :] = (sl * g).astype(bf16)
            else:
                slope[t, pl.ds(pl.multiple_of(i * rb, rb), rb), :] = sl

    def e_copy(t, r, c):
        cols = pl.ds(pl.multiple_of(c * CW, CW), CW)
        return rcopy(
            own_e.at[t, :, cols], peer_e.at[t, r - 1, :, cols],
            e_s.at[t, r - 1, c], e_r.at[t, r - 1, c], {"tp": (p + r) % TP},
        )

    def z_copy(t, c):
        cols = pl.ds(pl.multiple_of(c * CW, CW), CW)
        to = jnp.maximum(s - 1, 0)
        return rcopy(
            dxs.at[t, :, cols], dyn.at[t, :, cols], z_s.at[t, c], z_r.at[t, c], {"section": to}
        )

    def spread(t):
        du = rhs[2 * t, pl.ds(mine, n), :]
        u = prod[pl.ds(t * n, n), :]
        m = jnp.sum(du.astype(f32) * u, axis=-1, keepdims=True) / D
        iv = inv[t, :, 0:1]
        q_scale = iv * iv * m

        @pl.loop(0, CH)
        def _(c):
            cols = pl.ds(pl.multiple_of(c * CW, CW), CW)
            dh = lax.dot_general(
                rhs[2 * t, pl.ds(mine, n), :], wfull[cols, :], (((1,), (1,)), ((), ())),
                preferred_element_type=f32,
            )
            e = iv * (gain_ref[0:1, cols] * dh) - xt[t, :, cols].astype(f32) * q_scale
            own_e[t, :, cols] = e.astype(bf16)
            for r in range(1, TP):
                e_copy(t, r, c).start()

    def combine(t, c):
        cols = pl.ds(pl.multiple_of(c * CW, CW), CW)
        for r in range(1, TP):
            e_copy(t, r, c).wait_recv()
        total = own_e[t, :, cols].astype(f32)
        for r in range(1, TP):
            total = total + peer_e[t, r - 1, :, cols].astype(f32)
        dy = act[pl.ds(T * n, n), cols] if t == 0 else dyn[t - 1, :, cols]
        dxs[t, :, cols] = (dy.astype(f32) + total).astype(bf16)
        z_copy(t, c).start()

    parts = []
    for t in range(T):
        parts += [2 * t, 2 * t + 1] if t == 0 else [2 * t + 1, 2 * t]

    def own_rows(at):
        part = parts[at]
        l_pass(part)
        l_own(part).wait()
        l_copy(part, 0).wait_recv()
        for k in range(1, FS - 1):
            if is_split(part):
                for q in range(1, TP):
                    x_copy(part, k, q).wait_recv()
            else:
                l_copy(part, k).wait_recv()
        for o in range(1, NC):
            r_copy(part, o).wait_recv()
            r_copy(part, NC - 1 + o).start()
        r_copy(part, 0).wait_recv()
        for o in range(1, NC):
            r_copy(part, NC - 1 + o).wait_recv()
        final = at == len(parts) - 1

        @pl.loop(0, N // nw)
        def _(i):
            cols = pl.ds(pl.multiple_of(i * nw, nw), nw)
            d = jnp.dot(lta[part], rhs[part, :, cols], preferred_element_type=f32)
            if at > 0:
                d = acc[:, cols] + d
            if final:
                wg_ref[0, :, cols] = d.astype(bf16)
            else:
                acc[:, cols] = d

    for t in range(T):
        if t == 0:
            gelu_rows(0, True)
        r_ids = [0, 1] if t == 0 else [2 * t]

        @pl.when(s > 0)
        def _():
            spread(t)

        for part in r_ids:
            r_send(part)
        if t == 0:
            for later in range(1, T):
                gelu_rows(later, False)
                r_send(2 * later + 1)

        if t < T - 1:
            @pl.when(s == S - 1)
            def _():
                pltpu.make_async_copy(gtop_ref.at[t], dyn.at[t], topsem.at[t]).wait()

            gr = pl.ds(T * n, n)

            @pl.loop(0, CH + LAG)
            def _(i):
                @pl.when((i < CH) & (s > 0))
                def _():
                    combine(t, i)

                if t == 0:
                    @pl.when(i == CH // 2)
                    def _():
                        l_pass(0)

                    @pl.when(i == CH - 1)
                    def _():
                        l_pass(1)

                @pl.when(i >= LAG)
                def _():
                    c = i - LAG

                    @pl.when(s < S - 1)
                    def _():
                        z_copy(t, c).wait_recv()

                    cols = pl.ds(pl.multiple_of(c * CW, CW), CW)
                    d = dyn[t, :, cols]
                    lt[2 * t + 3, cols, :] = d.astype(f32).T.astype(bf16)
                    g = jnp.dot(d, wfull[cols, :], preferred_element_type=f32)

                    @pl.when(c == 0)
                    def _():
                        prod[gr, :] = g

                    @pl.when(c > 0)
                    def _():
                        prod[gr, :] += g

            l_send(2 * t + 3)

            @pl.loop(0, n // rb)
            def _(i):
                rows = pl.ds(pl.multiple_of(i * rb, rb), rb)
                g = prod[pl.ds(pl.multiple_of(T * n + i * rb, rb), rb), :]
                here = pl.ds(pl.multiple_of(mine + i * rb, rb), rb)
                rhs[2 * t + 2, here, :] = (slope[t + 1, rows, :] * g).astype(bf16)
        else:
            for at in range(max(2 * T - 2, 0)):
                own_rows(at)
            for part in SPLIT:
                l_pass(part)

            @pl.when(s > 0)
            def _():
                @pl.loop(0, CH)
                def _(c):
                    combine(t, c)

    for at in range(max(2 * T - 2, 0), 2 * T):
        own_rows(at)

    t = T - 1

    @pl.when(s == S - 1)
    def _():
        pltpu.make_async_copy(gtop_ref.at[t], dyn.at[t], topsem.at[t]).wait()

    @pl.when(s < S - 1)
    def _():
        @pl.loop(0, CH)
        def _(c):
            z_copy(t, c).wait_recv()

    out = pltpu.make_async_copy(dyn.at[t], held_ref.at[0], heldsem.at[0])
    out.start()

    for j in range(WCH):
        for k in range(2 * NC - 1):
            w_copy(k, j).wait_send()
    for part in range(2 * T):
        for k in range(FS - 1):
            l_copy(part, k).wait_send()
        if is_split(part):
            for k in range(1, FS - 1):
                for q in range(1, TP):
                    x_copy(part, k, q).wait_send()
        for k in range(2 * NC - 1):
            r_copy(part, k).wait_send()

    @pl.when(s > 0)
    def _():
        for t in range(T):
            @pl.loop(0, CH)
            def _(c):
                for r in range(1, TP):
                    e_copy(t, r, c).wait_send()
                z_copy(t, c).wait_send()

    out.wait()


def solution(mesh):
    S, FS, TP = mesh.shape["section"], mesh.shape["fsdp"], mesh.shape["tp"]

    def per_device(stash, grad_now, grad_top, order, gain, weight):
        MB, n, D = stash.shape[1:]
        T = grad_top.shape[0]
        wl, N = weight.shape[1:]
        NC = FS // 2
        CH = D // pick(D, (384, 256, 128))
        WCH = 4 if wl % 64 == 0 else 1
        K = 2 * NC - 1
        DMA = pltpu.SemaphoreType.DMA
        V = pltpu.VMEM
        any_ = pl.BlockSpec(memory_space=pl.ANY)
        peers = max(TP - 1, 1)
        held, wg = pl.pallas_call(
            functools.partial(kernel, S, FS, TP, T),
            out_shape=(
                jax.ShapeDtypeStruct((1, n, D), bf16),
                jax.ShapeDtypeStruct((1, wl, N), bf16),
            ),
            in_specs=[
                pl.BlockSpec(memory_space=pltpu.SMEM),
                pl.BlockSpec(memory_space=pltpu.VMEM),
                any_, any_, any_, any_,
            ],
            out_specs=(any_, pl.BlockSpec(memory_space=pltpu.VMEM)),
            scratch_shapes=[
                V((FS * wl, N), bf16),
                V((MB, n, D), bf16),
                V(((T + 1) * n, D), bf16),
                V((T, n, D), bf16),
                V((T, n, 128), f32),
                V((T, n, D), bf16),
                V((2 * T, D, n), bf16),
                V((2 * T, wl, FS * n), bf16),
                V((2 * T, FS * n, N), bf16),
                V(((T + 1) * n, N), f32),
                V((T, n, N), f32),
                V((T, n, D), bf16),
                V((T, peers, n, D), bf16),
                V((T, n, D), bf16),
                V((wl, N), f32),
                DMA((3,)), DMA((T,)), DMA((2 * T,)), DMA((1,)),
                DMA((K, WCH)), DMA((K, WCH)),
                DMA((2 * T, FS - 1)), DMA((2 * T, FS - 1)),
                DMA((2 * T, K)), DMA((2 * T, K)),
                DMA((T, peers, CH)), DMA((T, peers, CH)),
                DMA((T, CH)), DMA((T, CH)),
                DMA((2 * T, max(FS - 2, 1), peers)), DMA((2 * T, max(FS - 2, 1), peers)),
            ],
            compiler_params=pltpu.CompilerParams(
                collective_id=0, has_side_effects=True, vmem_limit_bytes=60 * 1024 * 1024
            ),
        )(order, gain, stash, grad_now, grad_top, weight)
        return held, wg.astype(f32)

    return jax.shard_map(
        per_device,
        mesh=mesh,
        in_specs=(
            P("section", None, "fsdp", None),
            P("section", "fsdp", None),
            P(None, "fsdp", None),
            P("section", None),
            P("section", None),
            P("section", "fsdp", "tp"),
        ),
        out_specs=(P("section", "fsdp", None), P("section", "fsdp", "tp")),
        check_vma=False,
    )
```
